128 devices in a mesh: dp: 4 (over z), col: 4 (over y), row: 8 (over x, core).
Axes of the slice: x: 4, y: 4, z: 4, core: 2. Of those that a mesh axis runs over, the one named last changes fastest.
Arguments:
- x_attn: bfloat16 [16384, 2048], P('dp', 'row')
- dy_attn: bfloat16 [16384, 2048], P('dp', 'col')
- x_mlp: bfloat16 [16384, 2048], P('dp', 'row')
- dy_gate: bfloat16 [16384, 5120], P('dp', 'col')
- dy_up: bfloat16 [16384, 5120], P('dp', 'col')
- h_mlp: bfloat16 [16384, 5120], P('dp', 'row')
- dy_out: bfloat16 [16384, 2048], P('dp', 'col')
- w_attn: float32 [2048, 2048], P('row', 'col')
- w_gate: float32 [2048, 5120], P('row', 'col')
- w_up: float32 [2048, 5120], P('row', 'col')
- w_down: float32 [5120, 2048], P('row', 'col')
- r_attn: float32 [2048], P('row')
- c_attn: float32 [2048], P('col')
- r_gate: float32 [2048], P('row')
- c_gate: float32 [5120], P('col')
- r_up: float32 [2048], P('row')
- c_up: float32 [5120], P('col')
- r_down: float32 [5120], P('row')
- c_down: float32 [2048], P('col')
- hyper_params: float32 [3], replicated
Outputs:
- output 1: float32 [2048, 2048], P('row', 'col')
- output 2: float32 [2048], P('row')
- output 3: float32 [2048], P('col')
- output 4: float32 [2048, 5120], P('row', 'col')
- output 5: float32 [2048], P('row')
- output 6: float32 [5120], P('col')
- output 7: float32 [2048, 5120], P('row', 'col')
- output 8: float32 [2048], P('row')
- output 9: float32 [5120], P('col')
- output 10: float32 [5120, 2048], P('row', 'col')
- output 11: float32 [5120], P('row')
- output 12: float32 [2048], P('col')
All inputs are finite; a program needn't handle non-finite values.
Results may differ from the reference program's by a relative error of at most 0.001.
Values are sent between devices in bfloat16 or wider.
A program may use at most 1 GiB of HBM per device.

```python
import jax
import jax.numpy as jnp

D_MODEL = 2048
D_FF = 5120
TOKENS = 16384

EPS_ONE = 1e-30
EPS_TWO = 1e-3


def draw_act(key, rows, cols, scale):
    k_val, k_slope, k_one, k_two = jax.random.split(key, 4)
    position = jnp.linspace(-1.0, 1.0, cols)
    slope_val = jax.random.uniform(k_slope, (), jnp.float32, 0.8, 1.2)
    up_scale = jnp.exp(0.5 * slope_val * position) * jax.random.uniform(k_one, (cols,), jnp.float32, 0.7, 1.3)
    down_scale = jnp.exp(-0.5 * slope_val * position) * jax.random.uniform(k_two, (cols,), jnp.float32, 0.7, 1.3)
    group_scale = jnp.stack([up_scale, down_scale])
    values = jax.random.normal(k_val, (2, rows // 2, cols), jnp.float32) * group_scale[:, None, :]
    return (values.reshape(rows, cols) * scale).astype(jnp.bfloat16)


def draw_weight(key, rows, cols):
    k_val, k_row, k_col = jax.random.split(key, 3)
    row_trend = jax.random.uniform(k_row, (), jnp.float32, 0.8, 1.2) * jnp.linspace(-0.5, 0.5, rows)
    col_trend = jax.random.uniform(k_col, (), jnp.float32, 0.8, 1.2) * jnp.linspace(-0.5, 0.5, cols)
    values = jax.random.normal(k_val, (rows, cols), jnp.float32) * jnp.exp(row_trend[:, None] + col_trend[None, :])
    return values * rows ** -0.5


def draw_stat(key, length):
    return jax.random.uniform(key, (length,), jnp.float32, 0.2, 0.8)


def setup_inputs(seed: int = 0) -> dict:
    key_list = jax.random.split(jax.random.key(seed), 20)
    dy_scale = TOKENS ** -0.5
    hyper_keys = jax.random.split(key_list[19], 3)
    hyper_params = jnp.stack([
        jax.random.uniform(hyper_keys[0], (), jnp.float32, 0.5, 0.9),
        jax.random.uniform(hyper_keys[1], (), jnp.float32, 0.5, 1.0),
        jax.random.uniform(hyper_keys[2], (), jnp.float32, 0.3, 0.6)])
    return {
        'x_attn': draw_act(key_list[0], TOKENS, D_MODEL, 1.0),
        'dy_attn': draw_act(key_list[1], TOKENS, D_MODEL, dy_scale),
        'x_mlp': draw_act(key_list[2], TOKENS, D_MODEL, 1.0),
        'dy_gate': draw_act(key_list[3], TOKENS, D_FF, dy_scale),
        'dy_up': draw_act(key_list[4], TOKENS, D_FF, dy_scale),
        'h_mlp': draw_act(key_list[5], TOKENS, D_FF, 1.0),
        'dy_out': draw_act(key_list[6], TOKENS, D_MODEL, dy_scale),
        'w_attn': draw_weight(key_list[7], D_MODEL, D_MODEL),
        'w_gate': draw_weight(key_list[8], D_MODEL, D_FF),
        'w_up': draw_weight(key_list[9], D_MODEL, D_FF),
        'w_down': draw_weight(key_list[10], D_FF, D_MODEL),
        'r_attn': draw_stat(key_list[11], D_MODEL),
        'c_attn': draw_stat(key_list[12], D_MODEL),
        'r_gate': draw_stat(key_list[13], D_MODEL),
        'c_gate': draw_stat(key_list[14], D_FF),
        'r_up': draw_stat(key_list[15], D_MODEL),
        'c_up': draw_stat(key_list[16], D_FF),
        'r_down': draw_stat(key_list[17], D_FF),
        'c_down': draw_stat(key_list[18], D_MODEL),
        'hyper_params': hyper_params,
    }


def adafactor_step(x_act, dy_act, weight, row_old, col_old, hyper_params):
    beta_two = hyper_params[0]
    rho_step = hyper_params[1]
    clip_thr = hyper_params[2]
    full_grad = jnp.dot(x_act.T, dy_act, preferred_element_type=jnp.float32)
    sq_grad = full_grad * full_grad + EPS_ONE
    new_row = beta_two * row_old + (1.0 - beta_two) * jnp.mean(sq_grad, axis=1)
    new_col = beta_two * col_old + (1.0 - beta_two) * jnp.mean(sq_grad, axis=0)
    row_total = jnp.sum(new_row)
    second_est = new_row[:, None] * new_col[None, :] / row_total
    update = full_grad / jnp.sqrt(second_est)
    upd_rms = jnp.sqrt(jnp.mean(update * update))
    update = update / jnp.maximum(1.0, upd_rms / clip_thr)
    w_rms = jnp.sqrt(jnp.mean(weight * weight))
    step_size = rho_step * jnp.maximum(EPS_TWO, w_rms)
    return (weight - step_size * update, new_row, new_col)


def reference(x_attn, dy_attn, x_mlp, dy_gate, dy_up, h_mlp, dy_out, w_attn, w_gate, w_up, w_down,
              r_attn, c_attn, r_gate, c_gate, r_up, c_up, r_down, c_down, hyper_params):
    attn_res = adafactor_step(x_attn, dy_attn, w_attn, r_attn, c_attn, hyper_params)
    gate_res = adafactor_step(x_mlp, dy_gate, w_gate, r_gate, c_gate, hyper_params)
    up_res = adafactor_step(x_mlp, dy_up, w_up, r_up, c_up, hyper_params)
    down_res = adafactor_step(h_mlp, dy_out, w_down, r_down, c_down, hyper_params)
    return (attn_res[0], attn_res[1], attn_res[2], gate_res[0], gate_res[1], gate_res[2],
            up_res[0], up_res[1], up_res[2], down_res[0], down_res[1], down_res[2])
```

```python
import functools
import jax
import jax.numpy as jnp
from jax import lax
from jax.experimental import pallas as pl
from jax.experimental.pallas import tpu as pltpu
from jax.sharding import PartitionSpec as P

EPS_ONE = 1e-30
EPS_TWO = 1e-3
LANES = 128
MESH = pl.DeviceIdType.MESH
N_MAT = 4
TOKEN_CHUNKS = 4


class Mat:
    def __init__(self, m, n, row_size, col_size, row_off, col_off):
        self.m, self.n = m, n
        self.mc = m // 8
        self.m_total, self.n_total = m * row_size, n * col_size
        self.rows = m // LANES
        self.row_off, self.col_off = row_off, col_off


def remote(src, dst, send_sem, recv_sem, axis, index):
    return pltpu.make_async_remote_copy(src_ref=src, dst_ref=dst, send_sem=send_sem, recv_sem=recv_sem,
                                        device_id={axis: index}, device_id_type=MESH)


def total(value):
    return jnp.sum(jnp.sum(value, axis=0, keepdims=True), axis=1, keepdims=True)


def kernel(mats, dp_size, col_size, row_size,
           x_attn, dy_attn, x_mlp, dy_gate, dy_up, h_mlp, dy_out,
           w0, w1, w2, w3, r0, r1, r2, r3, c0, c1, c2, c3, hyper,
           o0, o1, o2, o3, ro0, ro1, ro2, ro3, co0, co1, co2, co3,
           x_attn_v, dy_attn_v, x_mlp_v, dy_gate_v, dy_up_v, h_mlp_v, dy_out_v,
           wv0, wv1, wv2, wv3, gp0, gp1, gp2, gp3, gf0, gf1, gf2, gf3, rb0, rb1, rb2, rb3,
           r_old, c_old, r_new, c_new, b_row, a0, a1, a2, a3,
           cz, rz, cx, ry, sz, sy, sx,
           in_sem, w_sem, rc_sem, out_sem, rc_out_sem,
           rs_send, rs_recv, bc_send, bc_recv,
           z_send, z_recv, x_send, x_recv, y_send, y_recv):
    w_hbm = (w0, w1, w2, w3)
    r_hbm = (r0, r1, r2, r3)
    c_hbm = (c0, c1, c2, c3)
    w_out = (o0, o1, o2, o3)
    r_out = (ro0, ro1, ro2, ro3)
    c_out = (co0, co1, co2, co3)
    w_v = (wv0, wv1, wv2, wv3)
    gp = (gp0, gp1, gp2, gp3)
    gf = (gf0, gf1, gf2, gf3)
    rb = (rb0, rb1, rb2, rb3)
    acol = (a0, a1, a2, a3)
    z = lax.axis_index("dp")
    y = lax.axis_index("col")
    x = lax.axis_index("row")
    zp, zm, z2 = lax.rem(z + 1, 4), lax.rem(z + 3, 4), lax.rem(z + 2, 4)

    acts = ((x_attn, x_attn_v), (dy_attn, dy_attn_v), (x_mlp, x_mlp_v), (dy_gate, dy_gate_v),
            (dy_up, dy_up_v), (h_mlp, h_mlp_v), (dy_out, dy_out_v))
    groups = ((0, 1), (2, 3), (4,), (5, 6))
    tokens = x_attn.shape[0]
    tc = tokens // TOKEN_CHUNKS

    def act_copy(a, t):
        src, dst = acts[a]
        return pltpu.make_async_copy(src.at[pl.ds(t * tc, tc), :], dst.at[pl.ds(t * tc, tc), :], in_sem.at[a, t])

    for group in groups:
        for t in range(TOKEN_CHUNKS):
            for a in group:
                act_copy(a, t).start()
    w_copies = [pltpu.make_async_copy(w_hbm[k], w_v[k], w_sem.at[k]) for k in range(N_MAT)]
    rc_copies = []
    for k, mat in enumerate(mats):
        rc_copies.append(pltpu.make_async_copy(r_hbm[k], r_old.at[pl.ds(mat.row_off, mat.rows)], rc_sem.at[k]))
        rc_copies.append(pltpu.make_async_copy(c_hbm[k], c_old.at[:, pl.ds(mat.col_off, mat.n)], rc_sem.at[4 + k]))
    for copy in w_copies + rc_copies:
        copy.start()

    barrier = pltpu.get_barrier_semaphore()
    partners = 0
    for axis, me, size in (("dp", z, dp_size), ("col", y, col_size), ("row", x, row_size)):
        for d in range(1, size):
            pl.semaphore_signal(barrier, inc=1, device_id={axis: lax.rem(me + d, size)}, device_id_type=MESH)
            partners += 1

    operands = ((x_attn_v, dy_attn_v, (0, 1)), (x_mlp_v, dy_gate_v, (2, 3)),
                (x_mlp_v, dy_up_v, (4,)), (h_mlp_v, dy_out_v, (5, 6)))

    def matmul_chunk(k, t):
        x_ref, dy_ref, group = operands[k]
        mat = mats[k]
        for a in group:
            act_copy(a, t).wait()
        part = lax.dot_general(x_ref[pl.ds(t * tc, tc), :], dy_ref[pl.ds(t * tc, tc), :],
                               (((0,), (0,)), ((), ())), preferred_element_type=jnp.float32)
        part = part.reshape(8, mat.mc, mat.n)
        if t == 0:
            gp[k][...] = part
        else:
            gp[k][...] += part

    def cls(root, mirror):
        return 2 * root + mirror

    rs = {}

    def rs_copy(k, i, src, axis_index):
        rs[k, i] = remote(src, rb[k].at[i], rs_send.at[k, i], rs_recv.at[k, i], "dp", axis_index)
        rs[k, i].start()

    def rs_first(k):
        rs_copy(k, 0, gp[k].at[cls(z2, 0)], zm)
        rs_copy(k, 1, gp[k].at[cls(z2, 1)], zp)
        rs_copy(k, 2, gp[k].at[cls(zp, 0)], zp)
        rs_copy(k, 3, gp[k].at[cls(zm, 1)], zm)

    def rs_forward(k):
        rs[k, 0].wait_recv()
        rb[k][0] += gp[k][cls(zm, 0)]
        rs_copy(k, 4, rb[k].at[0], zm)
        rs[k, 1].wait_recv()
        rb[k][1] += gp[k][cls(zp, 1)]
        rs_copy(k, 5, rb[k].at[1], zp)

    def rs_finish(k):
        for i in (2, 4, 3, 5):
            rs[k, i].wait_recv()
        mat = mats[k]
        row_part = jnp.zeros((mat.mc, 1), jnp.float32)
        cols = jnp.zeros((1, mat.n), jnp.float32)
        row_iota = lax.broadcasted_iota(jnp.int32, (mat.mc, LANES), 0)
        lane_iota = lax.broadcasted_iota(jnp.int32, (mat.mc, LANES), 1)
        lines = [jnp.zeros((1, LANES), jnp.float32) for _ in range(mat.rows)]
        for mirror in range(2):
            own = cls(z, mirror)
            full = gp[k][own] + rb[k][2 + mirror] + rb[k][4 + mirror]
            gf[k][own] = full
            sq = full * full + EPS_ONE
            cols = cols + jnp.sum(sq, axis=0, keepdims=True)
            row_part = jnp.broadcast_to(jnp.sum(sq, axis=1, keepdims=True), (mat.mc, LANES))
            first = own * mat.mc
            for a in range(mat.rows):
                hit = (row_iota + first) == (lane_iota + a * LANES)
                lines[a] = lines[a] + jnp.sum(jnp.where(hit, row_part, 0.0), axis=0, keepdims=True)
        cz[z, :, pl.ds(mat.col_off, mat.n)] = cols
        for a in range(mat.rows):
            rz[z, mat.row_off + a] = lines[a]

    bc = {}

    def bc_copy(k, i, chunk, axis_index):
        bc[k, i] = remote(gf[k].at[chunk], gf[k].at[chunk], bc_send.at[k, i], bc_recv.at[k, i], "dp", axis_index)
        bc[k, i].start()

    def bc_first(k):
        bc_copy(k, 0, cls(z, 0), zp)
        bc_copy(k, 1, cls(z, 1), zm)
        bc_copy(k, 2, cls(z, 1), zp)
        bc_copy(k, 3, cls(z, 0), zm)

    def bc_forward(k):
        bc[k, 0].wait_recv()
        bc_copy(k, 4, cls(zm, 0), zp)
        bc[k, 1].wait_recv()
        bc_copy(k, 5, cls(zp, 1), zm)

    def exchange_start(axis, me, size, buf, send, recv, slot):
        copies = []
        for d in range(1, size):
            copies.append(remote(buf.at[me], buf.at[me], send.at[slot, d - 1], recv.at[slot, d - 1],
                                 axis, lax.rem(me + d, size)))
            copies[-1].start()
        return copies

    def recv_all(copies):
        for copy in copies:
            copy.wait_recv()

    for t in range(TOKEN_CHUNKS):
        matmul_chunk(0, t)
    pl.semaphore_wait(barrier, partners)
    rs_first(0)
    for t in range(TOKEN_CHUNKS):
        matmul_chunk(1, t)
    rs_forward(0)
    rs_first(1)
    for t in range(TOKEN_CHUNKS):
        matmul_chunk(2, t)
    rs_first(2)
    for t in range(TOKEN_CHUNKS):
        matmul_chunk(3, t)
    rs_forward(1)
    rs_first(3)
    rs_finish(0)
    for copy in w_copies + rc_copies:
        copy.wait()
    lane = lax.broadcasted_iota(jnp.int32, (1, LANES), 1)
    scal = jnp.zeros((1, LANES), jnp.float32)
    for k in range(N_MAT):
        for mirror in range(2):
            own_w = w_v[k][cls(z, mirror)]
            scal = jnp.where(lane == 4 + k, scal + total(own_w * own_w), scal)
    rs_forward(2)
    rs_finish(1)
    rs_forward(3)
    bc_first(0)
    rs_finish(2)
    rs_finish(3)
    hops = []
    zc = exchange_start("dp", z, dp_size, cz, z_send, z_recv, 0)
    zr = exchange_start("dp", z, dp_size, rz, z_send, z_recv, 1)
    bc_first(1)
    recv_all(zc)
    recv_all(zr)
    hops += zc + zr
    cx[x] = cz[0] + cz[1] + cz[2] + cz[3]
    ry[y] = rz[0] + rz[1] + rz[2] + rz[3]
    xc = exchange_start("row", x, row_size, cx, x_send, x_recv, 0)
    yr = exchange_start("col", y, col_size, ry, y_send, y_recv, 0)
    bc_forward(0)
    recv_all(xc)
    recv_all(yr)
    hops += xc + yr
    c_sum = cx[0]
    for i in range(1, row_size):
        c_sum = c_sum + cx[i]
    r_sum = ry[0]
    for i in range(1, col_size):
        r_sum = r_sum + ry[i]
    beta_two, rho_step, clip_thr = hyper[0], hyper[1], hyper[2]
    row_iota = lax.broadcasted_iota(jnp.int32, (LANES, LANES), 0)
    lane_iota = lax.broadcasted_iota(jnp.int32, (LANES, LANES), 1)
    eye = row_iota == lane_iota
    out_rc = []
    local_sum = []
    for k, mat in enumerate(mats):
        cs = slice(mat.col_off, mat.col_off + mat.n)
        new_c = beta_two * c_old[:, cs] + (1.0 - beta_two) * (c_sum[:, cs] * (1.0 / mat.m_total))
        c_new[:, cs] = new_c
        b_row[:, cs] = lax.rsqrt(new_c)
        out_rc.append(pltpu.make_async_copy(c_new.at[:, pl.ds(mat.col_off, mat.n)], c_out[k], rc_out_sem.at[4 + k]))
        lines = []
        for a in range(mat.rows):
            at = mat.row_off + a
            lines.append(beta_two * r_old[at] + (1.0 - beta_two) * (r_sum[at] * (1.0 / mat.n_total)))
            r_new[at] = lines[-1]
        out_rc.append(pltpu.make_async_copy(r_new.at[pl.ds(mat.row_off, mat.rows)], r_out[k], rc_out_sem.at[k]))
        s_loc = lines[0]
        for line in lines[1:]:
            s_loc = s_loc + line
        s_loc = jnp.sum(s_loc, axis=1, keepdims=True)
        local_sum.append(s_loc)
        for a in range(mat.rows):
            scaled = lax.rsqrt(lines[a] / s_loc)
            column = jnp.sum(jnp.where(eye, jnp.broadcast_to(scaled, (LANES, LANES)), 0.0), axis=1, keepdims=True)
            acol[k][pl.ds(a * LANES, LANES), :] = jnp.broadcast_to(column, (LANES, LANES))

    def scaled_tile(k, chunk, j):
        mat = mats[k]
        rows = pl.ds(pl.multiple_of(chunk * mat.mc, 8), mat.mc)
        cols = b_row[:, mat.col_off + j * LANES:mat.col_off + (j + 1) * LANES]
        return gf[k][chunk, :, j * LANES:(j + 1) * LANES] * acol[k][rows, :] * cols

    for k, mat in enumerate(mats):
        acc = jnp.zeros((mat.mc, LANES), jnp.float32)
        for mirror in range(2):
            for j in range(mat.n // LANES):
                upd = scaled_tile(k, cls(z, mirror), j)
                acc = acc + upd * upd
        scal = jnp.where(lane == k, total(acc), scal)
    sz[z] = scal
    zs = exchange_start("dp", z, dp_size, sz, z_send, z_recv, 2)
    bc_first(2)
    for copy in out_rc:
        copy.start()
    recv_all(zs)
    sy[y] = sz[0] + sz[1] + sz[2] + sz[3]
    ys = exchange_start("col", y, col_size, sy, y_send, y_recv, 1)
    bc_forward(1)
    bc_first(3)
    recv_all(ys)
    scal = sy[0]
    for i in range(1, col_size):
        scal = scal + sy[i]
    for k in range(N_MAT):
        scal = jnp.where(lane == 8 + k, jnp.broadcast_to(local_sum[k], (1, LANES)), scal)
    sx[x] = scal
    xs = exchange_start("row", x, row_size, sx, x_send, x_recv, 1)
    recv_all(xs)
    hops += zs + ys + xs
    table = jnp.concatenate([sx[i] for i in range(row_size)], axis=0)
    t_lane = lax.broadcasted_iota(jnp.int32, (row_size, LANES), 1)

    def pick(at):
        return jnp.sum(jnp.where(t_lane == at, table, 0.0), axis=1, keepdims=True)

    factors = []
    for k, mat in enumerate(mats):
        s_each = pick(8 + k)
        s_all = jnp.sum(s_each, axis=0, keepdims=True)
        count = 1.0 / (mat.m_total * mat.n_total)
        u_sq = jnp.sum((s_all / s_each) * pick(k), axis=0, keepdims=True)
        w_sq = jnp.sum(pick(4 + k), axis=0, keepdims=True)
        u_rms = jnp.sqrt(u_sq * count)
        w_rms = jnp.sqrt(w_sq * count)
        step = rho_step * jnp.maximum(EPS_TWO, w_rms) / jnp.maximum(1.0, u_rms / clip_thr)
        factors.append(step * jnp.sqrt(s_all / local_sum[k]))

    outs = []

    def update(k, chunk, slot):
        mat = mats[k]
        for j in range(mat.n // LANES):
            cols = slice(j * LANES, (j + 1) * LANES)
            w_v[k][chunk, :, cols] = w_v[k][chunk, :, cols] - factors[k] * scaled_tile(k, chunk, j)
        outs.append(pltpu.make_async_copy(w_v[k].at[chunk], w_out[k].at[chunk], out_sem.at[k, slot]))
        outs[-1].start()

    def update_own(k):
        update(k, cls(z, 0), 0)
        update(k, cls(z, 1), 1)

    def update_near(k):
        update(k, cls(zm, 0), 2)
        update(k, cls(zp, 1), 3)
        bc[k, 2].wait_recv()
        update(k, cls(zm, 1), 4)
        bc[k, 3].wait_recv()
        update(k, cls(zp, 0), 5)

    def update_far(k):
        bc[k, 4].wait_recv()
        update(k, cls(z2, 0), 6)
        bc[k, 5].wait_recv()
        update(k, cls(z2, 1), 7)

    bc_forward(2)
    for k in range(N_MAT):
        update_own(k)
    update_near(0)
    update_near(1)
    update_near(2)
    update_far(0)
    update_far(1)
    bc_forward(3)
    update_far(2)
    update_near(3)
    update_far(3)
    for copy in list(rs.values()) + list(bc.values()) + hops:
        copy.wait_send()
    for copy in outs + out_rc:
        copy.wait()


def fused_step(mats, dp_size, col_size, row_size, args):
    (x_attn, dy_attn, x_mlp, dy_gate, dy_up, h_mlp, dy_out, w_list, r_list, c_list, hyper) = args
    any_spec = pl.BlockSpec(memory_space=pl.ANY)
    f32 = jnp.float32
    w_in = [w.reshape(8, mat.mc, mat.n) for w, mat in zip(w_list, mats)]
    r_in = [r.reshape(mat.rows, 1, LANES) for r, mat in zip(r_list, mats)]
    c_in = [c.reshape(1, mat.n) for c, mat in zip(c_list, mats)]
    out_shape = ([jax.ShapeDtypeStruct(w.shape, f32) for w in w_in]
                 + [jax.ShapeDtypeStruct(r.shape, f32) for r in r_in]
                 + [jax.ShapeDtypeStruct(c.shape, f32) for c in c_in])
    acts = (x_attn, dy_attn, x_mlp, dy_gate, dy_up, h_mlp, dy_out)
    n_row = sum(mat.rows for mat in mats)
    n_col = sum(mat.n for mat in mats)
    scratch = ([pltpu.VMEM(a.shape, a.dtype) for a in acts]
               + [pltpu.VMEM((8, mat.mc, mat.n), f32) for mat in mats] * 3
               + [pltpu.VMEM((6, mat.mc, mat.n), f32) for mat in mats]
               + [pltpu.VMEM((n_row, 1, LANES), f32), pltpu.VMEM((1, n_col), f32)] * 2
               + [pltpu.VMEM((1, n_col), f32)]
               + [pltpu.VMEM((mat.m, LANES), f32) for mat in mats]
               + [pltpu.VMEM((dp_size, 1, n_col), f32), pltpu.VMEM((dp_size, n_row, 1, LANES), f32),
                  pltpu.VMEM((row_size, 1, n_col), f32), pltpu.VMEM((col_size, n_row, 1, LANES), f32),
                  pltpu.VMEM((dp_size, 1, LANES), f32), pltpu.VMEM((col_size, 1, LANES), f32),
                  pltpu.VMEM((row_size, 1, LANES), f32)]
               + [pltpu.SemaphoreType.DMA((7, TOKEN_CHUNKS)), pltpu.SemaphoreType.DMA((4,)),
                  pltpu.SemaphoreType.DMA((8,)), pltpu.SemaphoreType.DMA((4, 8)), pltpu.SemaphoreType.DMA((8,))]
               + [pltpu.SemaphoreType.DMA((4, 6))] * 4
               + [pltpu.SemaphoreType.DMA((3, dp_size - 1))] * 2
               + [pltpu.SemaphoreType.DMA((2, row_size - 1))] * 2
               + [pltpu.SemaphoreType.DMA((2, col_size - 1))] * 2)
    outs = pl.pallas_call(
        functools.partial(kernel, mats, dp_size, col_size, row_size),
        out_shape=out_shape,
        in_specs=[any_spec] * 19 + [pl.BlockSpec(memory_space=pltpu.SMEM)],
        out_specs=[any_spec] * 12,
        scratch_shapes=scratch,
        compiler_params=pltpu.CompilerParams(collective_id=0, has_side_effects=True, vmem_limit_bytes=67043328),
        name="adafactor_step",
    )(*acts, *w_in, *r_in, *c_in, hyper)
    new_w = [o.reshape(w.shape) for o, w in zip(outs[:4], w_list)]
    new_r = [o.reshape(r.shape) for o, r in zip(outs[4:8], r_list)]
    new_c = [o.reshape(c.shape) for o, c in zip(outs[8:], c_list)]
    return tuple(part for trio in zip(new_w, new_r, new_c) for part in trio)


def solution(mesh):
    row_size = mesh.shape['row']
    col_size = mesh.shape['col']
    dp_size = mesh.shape['dp']
    act_spec = P('dp', 'row')
    grad_spec = P('dp', 'col')
    w_spec = P('row', 'col')
    row_spec = P('row')
    col_spec = P('col')
    in_specs = (act_spec, grad_spec, act_spec, grad_spec, grad_spec, act_spec, grad_spec,
                w_spec, w_spec, w_spec, w_spec,
                row_spec, col_spec, row_spec, col_spec, row_spec, col_spec, row_spec, col_spec, P())
    out_specs = (w_spec, row_spec, col_spec) * 4

    def per_device(x_attn, dy_attn, x_mlp, dy_gate, dy_up, h_mlp, dy_out, w_attn, w_gate, w_up, w_down,
                   r_attn, c_attn, r_gate, c_gate, r_up, c_up, r_down, c_down, hyper_params):
        w_list = (w_attn, w_gate, w_up, w_down)
        mats = []
        row_off = col_off = 0
        for w in w_list:
            mats.append(Mat(w.shape[0], w.shape[1], row_size, col_size, row_off, col_off))
            row_off += mats[-1].rows
            col_off += mats[-1].n
        return fused_step(mats, dp_size, col_size, row_size,
                          (x_attn, dy_attn, x_mlp, dy_gate, dy_up, h_mlp, dy_out, w_list,
                           (r_attn, r_gate, r_up, r_down), (c_attn, c_gate, c_up, c_down), hyper_params))

    return jax.shard_map(per_device, mesh=mesh, in_specs=in_specs, out_specs=out_specs, check_vma=False)
```

```python
import functools
import jax
import jax.numpy as jnp
from jax import lax
from jax.experimental import pallas as pl
from jax.experimental.pallas import tpu as pltpu
from jax.sharding import PartitionSpec as P

EPS_ONE = 1e-30
EPS_TWO = 1e-3
LANES = 128
MESH = pl.DeviceIdType.MESH
N_MAT = 4
TOKEN_CHUNKS = 4
VMEM_LIMIT = 58 * 1024 * 1024
WRITE_LIMIT = 16 * 1024 * 1024


class Mat:
    def __init__(self, m, n, row_size, col_size, row_off, col_off):
        self.m, self.n = m, n
        self.mc = m // 8
        self.m_total, self.n_total = m * row_size, n * col_size
        self.rows = m // LANES
        self.row_off, self.col_off = row_off, col_off


def remote(src, dst, send_sem, recv_sem, axis, index):
    return pltpu.make_async_remote_copy(src_ref=src, dst_ref=dst, send_sem=send_sem, recv_sem=recv_sem,
                                        device_id={axis: index}, device_id_type=MESH)


def total(value):
    return jnp.sum(jnp.sum(value, axis=0, keepdims=True), axis=1, keepdims=True)


def kernel(mats, dp_size, col_size, row_size,
           x_attn, dy_attn, x_mlp, dy_gate, dy_up, h_mlp, dy_out,
           w0, w1, w2, w3, r0, r1, r2, r3, c0, c1, c2, c3, hyper,
           wv0, wv1, wv2, wv3, r_new, c_new,
           x_attn_v, dy_attn_v, x_mlp_v, dy_gate_v, dy_up_v, h_mlp_v, dy_out_v,
           gp0, gp1, gp2, gp3, gf0, gf1, gf2, gf3, rb0, rb1, rb2, rb3,
           r_old, c_old, b_row, a0, a1, a2, a3,
           cz, rz, cx, ry, sz, sy, sx,
           in_sem, w_sem, r_sem, c_sem,
           rs_send, rs_recv, bc_send, bc_recv,
           z_send, z_recv, x_send, x_recv, y_send, y_recv):
    w_hbm = (w0, w1, w2, w3)
    r_hbm = (r0, r1, r2, r3)
    c_hbm = (c0, c1, c2, c3)
    w_v = (wv0, wv1, wv2, wv3)
    gp = (gp0, gp1, gp2, gp3)
    gf = (gf0, gf1, gf2, gf3)
    rb = (rb0, rb1, rb2, rb3)
    acol = (a0, a1, a2, a3)
    z = lax.axis_index("dp")
    y = lax.axis_index("col")
    x = lax.axis_index("row")
    zp, zm, z2 = lax.rem(z + 1, 4), lax.rem(z + 3, 4), lax.rem(z + 2, 4)

    acts = ((x_attn, x_attn_v), (dy_attn, dy_attn_v), (x_mlp, x_mlp_v), (dy_gate, dy_gate_v),
            (dy_up, dy_up_v), (h_mlp, h_mlp_v), (dy_out, dy_out_v))
    groups = ((0, 1), (2, 3), (4,), (5, 6))
    tokens = x_attn.shape[0]
    tc = tokens // TOKEN_CHUNKS

    def act_copy(a, t):
        src, dst = acts[a]
        return pltpu.make_async_copy(src.at[pl.ds(t * tc, tc), :], dst.at[pl.ds(t * tc, tc), :], in_sem.at[a, t])

    for group in groups:
        for t in range(TOKEN_CHUNKS):
            for a in group:
                act_copy(a, t).start()
    w_copies = [pltpu.make_async_copy(w_hbm[k], w_v[k], w_sem.at[k]) for k in range(N_MAT)]
    rc_copies = []
    for k, mat in enumerate(mats):
        for a in range(mat.rows):
            at = mat.row_off + a
            rc_copies.append(pltpu.make_async_copy(r_hbm[k].at[pl.ds(a * LANES, LANES)], r_old.at[at, 0], r_sem.at[at]))
        rc_copies.append(pltpu.make_async_copy(c_hbm[k], c_old.at[0, pl.ds(mat.col_off, mat.n)], c_sem.at[k]))
    for copy in w_copies + rc_copies:
        copy.start()

    barrier = pltpu.get_barrier_semaphore()
    partners = 0
    for axis, me, size in (("dp", z, dp_size), ("col", y, col_size), ("row", x, row_size)):
        for d in range(1, size):
            pl.semaphore_signal(barrier, inc=1, device_id={axis: lax.rem(me + d, size)}, device_id_type=MESH)
            partners += 1

    operands = ((x_attn_v, dy_attn_v, (0, 1)), (x_mlp_v, dy_gate_v, (2, 3)),
                (x_mlp_v, dy_up_v, (4,)), (h_mlp_v, dy_out_v, (5, 6)))

    def matmul_chunk(k, t):
        x_ref, dy_ref, group = operands[k]
        mat = mats[k]
        for a in group:
            act_copy(a, t).wait()
        part = lax.dot_general(x_ref[pl.ds(t * tc, tc), :], dy_ref[pl.ds(t * tc, tc), :],
                               (((0,), (0,)), ((), ())), preferred_element_type=jnp.float32)
        part = part.reshape(8, mat.mc, mat.n)
        if t == 0:
            gp[k][...] = part
        else:
            gp[k][...] += part

    def cls(root, mirror):
        return 2 * root + mirror

    rs = {}

    def rs_copy(k, i, src, axis_index):
        rs[k, i] = remote(src, rb[k].at[i], rs_send.at[k, i], rs_recv.at[k, i], "dp", axis_index)
        rs[k, i].start()

    def rs_first(k):
        rs_copy(k, 0, gp[k].at[cls(z2, 0)], zm)
        rs_copy(k, 1, gp[k].at[cls(z2, 1)], zp)
        rs_copy(k, 2, gp[k].at[cls(zp, 0)], zp)
        rs_copy(k, 3, gp[k].at[cls(zm, 1)], zm)

    def rs_forward(k):
        rs[k, 0].wait_recv()
        rb[k][0] += gp[k][cls(zm, 0)]
        rs_copy(k, 4, rb[k].at[0], zm)
        rs[k, 1].wait_recv()
        rb[k][1] += gp[k][cls(zp, 1)]
        rs_copy(k, 5, rb[k].at[1], zp)

    def rs_finish(k):
        for i in (2, 4, 3, 5):
            rs[k, i].wait_recv()
        mat = mats[k]
        row_part = jnp.zeros((mat.mc, 1), jnp.float32)
        cols = jnp.zeros((1, mat.n), jnp.float32)
        row_iota = lax.broadcasted_iota(jnp.int32, (mat.mc, LANES), 0)
        lane_iota = lax.broadcasted_iota(jnp.int32, (mat.mc, LANES), 1)
        lines = [jnp.zeros((1, LANES), jnp.float32) for _ in range(mat.rows)]
        for mirror in range(2):
            own = cls(z, mirror)
            full = gp[k][own] + rb[k][2 + mirror] + rb[k][4 + mirror]
            gf[k][own] = full
            sq = full * full + EPS_ONE
            cols = cols + jnp.sum(sq, axis=0, keepdims=True)
            row_part = jnp.broadcast_to(jnp.sum(sq, axis=1, keepdims=True), (mat.mc, LANES))
            first = own * mat.mc
            for a in range(mat.rows):
                hit = (row_iota + first) == (lane_iota + a * LANES)
                lines[a] = lines[a] + jnp.sum(jnp.where(hit, row_part, 0.0), axis=0, keepdims=True)
        cz[z, :, pl.ds(mat.col_off, mat.n)] = cols
        for a in range(mat.rows):
            rz[z, mat.row_off + a] = lines[a]

    bc = {}

    def bc_copy(k, i, chunk, axis_index):
        bc[k, i] = remote(gf[k].at[chunk], gf[k].at[chunk], bc_send.at[k, i], bc_recv.at[k, i], "dp", axis_index)
        bc[k, i].start()

    def bc_first(k):
        bc_copy(k, 0, cls(z, 0), zp)
        bc_copy(k, 1, cls(z, 1), zm)
        bc_copy(k, 2, cls(z, 1), zp)
        bc_copy(k, 3, cls(z, 0), zm)

    def bc_forward(k):
        bc[k, 0].wait_recv()
        bc_copy(k, 4, cls(zm, 0), zp)
        bc[k, 1].wait_recv()
        bc_copy(k, 5, cls(zp, 1), zm)

    def exchange_start(axis, me, size, buf, send, recv, slot):
        copies = []
        for d in range(1, size):
            copies.append(remote(buf.at[me], buf.at[me], send.at[slot, d - 1], recv.at[slot, d - 1],
                                 axis, lax.rem(me + d, size)))
            copies[-1].start()
        return copies

    def recv_all(copies):
        for copy in copies:
            copy.wait_recv()

    for t in range(TOKEN_CHUNKS):
        matmul_chunk(0, t)
    pl.semaphore_wait(barrier, partners)
    rs_first(0)
    for t in range(TOKEN_CHUNKS):
        matmul_chunk(1, t)
    rs_forward(0)
    rs_first(1)
    for t in range(TOKEN_CHUNKS):
        matmul_chunk(2, t)
    rs_first(2)
    for t in range(TOKEN_CHUNKS):
        matmul_chunk(3, t)
    rs_forward(1)
    rs_first(3)
    rs_finish(0)
    for copy in w_copies + rc_copies:
        copy.wait()
    lane = lax.broadcasted_iota(jnp.int32, (1, LANES), 1)
    scal = jnp.zeros((1, LANES), jnp.float32)
    for k in range(N_MAT):
        for mirror in range(2):
            own_w = w_v[k][cls(z, mirror)]
            scal = jnp.where(lane == 4 + k, scal + total(own_w * own_w), scal)
    rs_forward(2)
    rs_finish(1)
    rs_forward(3)
    bc_first(0)
    rs_finish(2)
    rs_finish(3)
    hops = []
    zc = exchange_start("dp", z, dp_size, cz, z_send, z_recv, 0)
    zr = exchange_start("dp", z, dp_size, rz, z_send, z_recv, 1)
    bc_first(1)
    recv_all(zc)
    recv_all(zr)
    hops += zc + zr
    cx[x] = cz[0] + cz[1] + cz[2] + cz[3]
    ry[y] = rz[0] + rz[1] + rz[2] + rz[3]
    xc = exchange_start("row", x, row_size, cx, x_send, x_recv, 0)
    yr = exchange_start("col", y, col_size, ry, y_send, y_recv, 0)
    bc_forward(0)
    recv_all(xc)
    recv_all(yr)
    hops += xc + yr
    c_sum = cx[0]
    for i in range(1, row_size):
        c_sum = c_sum + cx[i]
    r_sum = ry[0]
    for i in range(1, col_size):
        r_sum = r_sum + ry[i]
    beta_two, rho_step, clip_thr = hyper[0], hyper[1], hyper[2]
    row_iota = lax.broadcasted_iota(jnp.int32, (LANES, LANES), 0)
    lane_iota = lax.broadcasted_iota(jnp.int32, (LANES, LANES), 1)
    eye = row_iota == lane_iota
    local_sum = []
    for k, mat in enumerate(mats):
        cs = slice(mat.col_off, mat.col_off + mat.n)
        new_c = beta_two * c_old[:, cs] + (1.0 - beta_two) * (c_sum[:, cs] * (1.0 / mat.m_total))
        c_new[:, cs] = new_c
        b_row[:, cs] = lax.rsqrt(new_c)
        lines = []
        for a in range(mat.rows):
            at = mat.row_off + a
            lines.append(beta_two * r_old[at] + (1.0 - beta_two) * (r_sum[at] * (1.0 / mat.n_total)))
            r_new[at] = lines[-1]
        s_loc = lines[0]
        for line in lines[1:]:
            s_loc = s_loc + line
        s_loc = jnp.sum(s_loc, axis=1, keepdims=True)
        local_sum.append(s_loc)
        for a in range(mat.rows):
            scaled = lax.rsqrt(lines[a] / s_loc)
            column = jnp.sum(jnp.where(eye, jnp.broadcast_to(scaled, (LANES, LANES)), 0.0), axis=1, keepdims=True)
            acol[k][pl.ds(a * LANES, LANES), :] = jnp.broadcast_to(column, (LANES, LANES))

    def scaled_tile(k, chunk, j):
        mat = mats[k]
        rows = pl.ds(pl.multiple_of(chunk * mat.mc, 8), mat.mc)
        cols = b_row[:, mat.col_off + j * LANES:mat.col_off + (j + 1) * LANES]
        return gf[k][chunk, :, j * LANES:(j + 1) * LANES] * acol[k][rows, :] * cols

    for k, mat in enumerate(mats):
        acc = jnp.zeros((mat.mc, LANES), jnp.float32)
        for mirror in range(2):
            for j in range(mat.n // LANES):
                upd = scaled_tile(k, cls(z, mirror), j)
                acc = acc + upd * upd
        scal = jnp.where(lane == k, total(acc), scal)
    sz[z] = scal
    zs = exchange_start("dp", z, dp_size, sz, z_send, z_recv, 2)
    bc_first(2)
    recv_all(zs)
    sy[y] = sz[0] + sz[1] + sz[2] + sz[3]
    ys = exchange_start("col", y, col_size, sy, y_send, y_recv, 1)
    bc_forward(1)
    bc_first(3)
    recv_all(ys)
    scal = sy[0]
    for i in range(1, col_size):
        scal = scal + sy[i]
    for k in range(N_MAT):
        scal = jnp.where(lane == 8 + k, jnp.broadcast_to(local_sum[k], (1, LANES)), scal)
    sx[x] = scal
    xs = exchange_start("row", x, row_size, sx, x_send, x_recv, 1)
    recv_all(xs)
    hops += zs + ys + xs
    table = jnp.concatenate([sx[i] for i in range(row_size)], axis=0)
    t_lane = lax.broadcasted_iota(jnp.int32, (row_size, LANES), 1)

    def pick(at):
        return jnp.sum(jnp.where(t_lane == at, table, 0.0), axis=1, keepdims=True)

    factors = []
    for k, mat in enumerate(mats):
        s_each = pick(8 + k)
        s_all = jnp.sum(s_each, axis=0, keepdims=True)
        count = 1.0 / (mat.m_total * mat.n_total)
        u_sq = jnp.sum((s_all / s_each) * pick(k), axis=0, keepdims=True)
        w_sq = jnp.sum(pick(4 + k), axis=0, keepdims=True)
        u_rms = jnp.sqrt(u_sq * count)
        w_rms = jnp.sqrt(w_sq * count)
        step = rho_step * jnp.maximum(EPS_TWO, w_rms) / jnp.maximum(1.0, u_rms / clip_thr)
        factors.append(step * jnp.sqrt(s_all / local_sum[k]))

    def update(k, chunk):
        mat = mats[k]
        for j in range(mat.n // LANES):
            cols = slice(j * LANES, (j + 1) * LANES)
            w_v[k][chunk, :, cols] = w_v[k][chunk, :, cols] - factors[k] * scaled_tile(k, chunk, j)

    def update_own(k):
        update(k, cls(z, 0))
        update(k, cls(z, 1))

    def update_near(k):
        update(k, cls(zm, 0))
        update(k, cls(zp, 1))
        bc[k, 2].wait_recv()
        update(k, cls(zm, 1))
        bc[k, 3].wait_recv()
        update(k, cls(zp, 0))

    def update_far(k):
        bc[k, 4].wait_recv()
        update(k, cls(z2, 0))
        bc[k, 5].wait_recv()
        update(k, cls(z2, 1))

    bc_forward(2)
    for k in range(N_MAT):
        update_own(k)
    update_near(0)
    update_near(1)
    update_near(2)
    update_far(0)
    update_far(1)
    bc_forward(3)
    update_far(2)
    update_near(3)
    update_far(3)
    for copy in list(rs.values()) + list(bc.values()) + hops:
        copy.wait_send()


def write_kernel(mats, w0, w1, w2, w3, r_new, c_new,
                 o0, o1, o2, o3, ro0, ro1, ro2, ro3, co0, co1, co2, co3, w_sem, r_sem, c_sem):
    copies = [pltpu.make_async_copy(src, dst, w_sem.at[k])
              for k, (src, dst) in enumerate(zip((w0, w1, w2, w3), (o0, o1, o2, o3)))]
    for k, mat in enumerate(mats):
        r_out = (ro0, ro1, ro2, ro3)[k]
        c_out = (co0, co1, co2, co3)[k]
        for a in range(mat.rows):
            at = mat.row_off + a
            copies.append(pltpu.make_async_copy(r_new.at[at, 0], r_out.at[pl.ds(a * LANES, LANES)], r_sem.at[at]))
        copies.append(pltpu.make_async_copy(c_new.at[0, pl.ds(mat.col_off, mat.n)], c_out, c_sem.at[k]))
    for copy in copies:
        copy.start()
    for copy in copies:
        copy.wait()


def fused_step(mats, dp_size, col_size, row_size, args):
    (x_attn, dy_attn, x_mlp, dy_gate, dy_up, h_mlp, dy_out, w_list, r_list, c_list, hyper) = args
    any_spec = pl.BlockSpec(memory_space=pl.ANY)
    vmem_spec = pl.BlockSpec(memory_space=pltpu.VMEM)
    f32 = jnp.float32
    w_in = [w.reshape(8, mat.mc, mat.n) for w, mat in zip(w_list, mats)]
    acts = (x_attn, dy_attn, x_mlp, dy_gate, dy_up, h_mlp, dy_out)
    n_row = sum(mat.rows for mat in mats)
    n_col = sum(mat.n for mat in mats)
    w_shape = [jax.ShapeDtypeStruct(w.shape, f32) for w in w_in]
    w_held = [pltpu.VMEM(w.shape, f32) for w in w_in]
    packed_shape = [pltpu.VMEM((n_row, 1, LANES), f32), pltpu.VMEM((1, n_col), f32)]
    scratch = ([pltpu.VMEM(a.shape, a.dtype) for a in acts]
               + [pltpu.VMEM((8, mat.mc, mat.n), f32) for mat in mats] * 2
               + [pltpu.VMEM((6, mat.mc, mat.n), f32) for mat in mats]
               + [pltpu.VMEM((n_row, 1, LANES), f32), pltpu.VMEM((1, n_col), f32), pltpu.VMEM((1, n_col), f32)]
               + [pltpu.VMEM((mat.m, LANES), f32) for mat in mats]
               + [pltpu.VMEM((dp_size, 1, n_col), f32), pltpu.VMEM((dp_size, n_row, 1, LANES), f32),
                  pltpu.VMEM((row_size, 1, n_col), f32), pltpu.VMEM((col_size, n_row, 1, LANES), f32),
                  pltpu.VMEM((dp_size, 1, LANES), f32), pltpu.VMEM((col_size, 1, LANES), f32),
                  pltpu.VMEM((row_size, 1, LANES), f32)]
               + [pltpu.SemaphoreType.DMA((7, TOKEN_CHUNKS)), pltpu.SemaphoreType.DMA((4,)),
                  pltpu.SemaphoreType.DMA((n_row,)), pltpu.SemaphoreType.DMA((4,))]
               + [pltpu.SemaphoreType.DMA((4, 6))] * 4
               + [pltpu.SemaphoreType.DMA((3, dp_size - 1))] * 2
               + [pltpu.SemaphoreType.DMA((2, row_size - 1))] * 2
               + [pltpu.SemaphoreType.DMA((2, col_size - 1))] * 2)
    held = pl.pallas_call(
        functools.partial(kernel, mats, dp_size, col_size, row_size),
        out_shape=w_held + packed_shape,
        in_specs=[any_spec] * 19 + [pl.BlockSpec(memory_space=pltpu.SMEM)],
        out_specs=[vmem_spec] * 6,
        scratch_shapes=scratch,
        compiler_params=pltpu.CompilerParams(collective_id=0, has_side_effects=True, vmem_limit_bytes=VMEM_LIMIT),
        name="adafactor_step",
    )(*acts, *w_in, *r_list, *c_list, hyper)
    outs = pl.pallas_call(
        functools.partial(write_kernel, mats),
        out_shape=(w_shape + [jax.ShapeDtypeStruct(r.shape, f32) for r in r_list]
                   + [jax.ShapeDtypeStruct(c.shape, f32) for c in c_list]),
        in_specs=[vmem_spec] * 6,
        out_specs=[any_spec] * 12,
        scratch_shapes=[pltpu.SemaphoreType.DMA((4,)), pltpu.SemaphoreType.DMA((n_row,)), pltpu.SemaphoreType.DMA((4,))],
        compiler_params=pltpu.CompilerParams(vmem_limit_bytes=WRITE_LIMIT),
        name="write_out",
    )(*held)
    new_w = [o.reshape(w.shape) for o, w in zip(outs[:4], w_list)]
    return tuple(part for trio in zip(new_w, outs[4:8], outs[8:]) for part in trio)


def solution(mesh):
    row_size = mesh.shape['row']
    col_size = mesh.shape['col']
    dp_size = mesh.shape['dp']
    act_spec = P('dp', 'row')
    grad_spec = P('dp', 'col')
    w_spec = P('row', 'col')
    row_spec = P('row')
    col_spec = P('col')
    in_specs = (act_spec, grad_spec, act_spec, grad_spec, grad_spec, act_spec, grad_spec,
                w_spec, w_spec, w_spec, w_spec,
                row_spec, col_spec, row_spec, col_spec, row_spec, col_spec, row_spec, col_spec, P())
    out_specs = (w_spec, row_spec, col_spec) * 4

    def per_device(x_attn, dy_attn, x_mlp, dy_gate, dy_up, h_mlp, dy_out, w_attn, w_gate, w_up, w_down,
                   r_attn, c_attn, r_gate, c_gate, r_up, c_up, r_down, c_down, hyper_params):
        w_list = (w_attn, w_gate, w_up, w_down)
        mats = []
        row_off = col_off = 0
        for w in w_list:
            mats.append(Mat(w.shape[0], w.shape[1], row_size, col_size, row_off, col_off))
            row_off += mats[-1].rows
            col_off += mats[-1].n
        return fused_step(mats, dp_size, col_size, row_size,
                          (x_attn, dy_attn, x_mlp, dy_gate, dy_up, h_mlp, dy_out, w_list,
                           (r_attn, r_gate, r_up, r_down), (c_attn, c_gate, c_up, c_down), hyper_params))

    return jax.shard_map(per_device, mesh=mesh, in_specs=in_specs, out_specs=out_specs, check_vma=False)
```

```python
import functools
import math
import jax
import jax.numpy as jnp
from jax import lax
from jax.experimental import pallas as pl
from jax.experimental.pallas import tpu as pltpu
from jax.sharding import PartitionSpec as P

EPS_ONE = 1e-30
EPS_TWO = 1e-3
LANES = 128
MESH = pl.DeviceIdType.MESH
N_MAT = 4
VMEM_LIMIT = 58 * 1024 * 1024
WRITE_LIMIT = 16 * 1024 * 1024
PIECES = ((0, 4, 4, False), (1, 4, 2, False), (1, 6, 1, False), (2, 6, 1, False), (2, 4, 1, True), (3, 4, 2, False))


class Mat:
    def __init__(self, m, n, row_size, col_size, row_off, col_off):
        self.m, self.n = m, n
        self.mc = m // 8
        self.m_total, self.n_total = m * row_size, n * col_size
        self.rows = m // LANES
        self.row_off, self.col_off = row_off, col_off


class Piece:
    def __init__(self, k, mat, lo, width, chunks, bent):
        self.k, self.mat, self.lo, self.width, self.chunks, self.bent = k, mat, lo, width, chunks, bent
        self.mc = mat.mc
        self.col_off = mat.col_off + lo
        self.tiles = width // LANES


def remote(src, dst, send_sem, recv_sem, axis, index):
    return pltpu.make_async_remote_copy(src_ref=src, dst_ref=dst, send_sem=send_sem, recv_sem=recv_sem,
                                        device_id={axis: index}, device_id_type=MESH)


def wait_bytes(ref, sem):
    pltpu.make_async_copy(ref, ref, sem).wait()


def size_of(ref):
    return math.prod(ref.shape) * jnp.dtype(ref.dtype).itemsize


def total(value):
    return jnp.sum(jnp.sum(value, axis=0, keepdims=True), axis=1, keepdims=True)


def lanes(at):
    return slice(at * LANES, (at + 1) * LANES)


def kernel(mats, pieces, dp_size, col_size, row_size, *refs):
    refs = list(refs)

    def take(count):
        part = refs[:count]
        del refs[:count]
        return part

    n_p = len(pieces)
    acts = take(7)
    w_hbm, r_hbm, c_hbm = take(N_MAT), take(N_MAT), take(N_MAT)
    hyper_hbm, = take(1)
    w_v = take(N_MAT)
    stat_new, = take(1)
    acts_v = take(7)
    x_turn, = take(1)
    gp, rb, gf, acol = take(n_p), take(n_p), take(N_MAT), take(N_MAT)
    hyper, stat_old, b_row, c_own, c_in, r_in, r_own, z_in, c_all, sz, sy, sx = take(12)
    ruler, in_sem, w_sem, st_sem, hyper_sem, rs_send, rs_mid, rs_root, bc_send, bc_fwd, bc_near, bc_last, bc_far, bc_more, ex_send, ex_recv = take(16)
    n_row = sum(mat.m for mat in mats)
    c_len = c_own.shape[2]
    z = lax.axis_index("dp")
    y = lax.axis_index("col")
    x = lax.axis_index("row")
    zp, zm, z2 = lax.rem(z + 1, 4), lax.rem(z + 3, 4), lax.rem(z + 2, 4)
    tokens = acts[0].shape[0]

    def wait_count(size, sem):
        rows = ruler if size <= size_of(ruler) else acts_v[3].at[:, pl.ds(0, 1024)]
        wait_bytes(rows.at[pl.ds(0, size * rows.shape[0] // size_of(rows))], sem)

    x_of = (0, 2, 2, 5)
    dy_of = (1, 3, 4, 6)
    groups = {}

    def load(a, lo, width, t, chunks, sem):
        tc = tokens // chunks
        at = (pl.ds(t * tc, tc), pl.ds(lo, width))
        pltpu.make_async_copy(acts[a].at[at], acts_v[a].at[at], sem).start()
        return tc * width * acts[a].dtype.itemsize

    for p, piece in enumerate(pieces):
        xa, ya = x_of[piece.k], dy_of[piece.k]
        new_x = piece.lo == 0 and x_of.index(xa) == piece.k
        chunks = piece.chunks
        for t in range(chunks):
            sem = in_sem.at[len(groups)]
            size = load(xa, 0, acts[xa].shape[1], t, chunks, sem) if new_x else 0
            groups[p, t] = (size + load(ya, piece.lo, piece.width, t, chunks, sem), sem)
    for k in range(N_MAT):
        pltpu.make_async_copy(w_hbm[k], w_v[k], w_sem).start()
    hyper_copy = pltpu.make_async_copy(hyper_hbm, hyper, hyper_sem)
    hyper_copy.start()
    for k, mat in enumerate(mats):
        pltpu.make_async_copy(r_hbm[k], stat_old.at[0, pl.ds(mat.row_off * LANES, mat.m)], st_sem).start()
        pltpu.make_async_copy(c_hbm[k], stat_old.at[0, pl.ds(n_row + mat.col_off, mat.n)], st_sem).start()

    barrier = pltpu.get_barrier_semaphore()
    partners = 0
    for axis, me, size in (("dp", z, dp_size), ("col", y, col_size), ("row", x, row_size)):
        for d in range(1, size):
            pl.semaphore_signal(barrier, inc=1, device_id={axis: lax.rem(me + d, size)}, device_id_type=MESH)
            partners += 1

    def matmul_chunk(p, t):
        piece = pieces[p]
        wait_count(*groups[p, t])
        tc = tokens // piece.chunks
        at = pl.ds(t * tc, tc)
        xa = x_of[piece.k]
        if piece.k in (0, 1) and piece.lo == 0:
            x_turn[:, at] = acts_v[xa][at, :].T
        if piece.k == 3:
            left, contract = acts_v[xa][at, :], 0
        else:
            left, contract = x_turn[:, at], 1
        part = lax.dot_general(left, acts_v[dy_of[piece.k]][at, pl.ds(piece.lo, piece.width)],
                               (((contract,), (0,)), ((), ())), preferred_element_type=jnp.float32)
        part = part.reshape(8, piece.mc, piece.width)
        if t == 0:
            gp[p][...] = part
        else:
            gp[p][...] += part

    def own_lines(root):
        return [mat.row_off + root // 2 for mat in mats[:-1]] + [mats[-1].row_off + root + i for i in range(2)]

    def cls(root, mirror):
        return 2 * root + mirror

    def rs_copy(p, i, src, axis_index, recv_sem):
        remote(src, rb[p].at[i], rs_send, recv_sem, "dp", axis_index).start()

    def rs_first(p):
        bent = pieces[p].bent
        inner = (z == 1) | (z == 2)
        to_a, slot_a = (jnp.where(inner, zp, zm), jnp.where(inner, 6, 0)) if bent else (zm, 0)
        to_b, slot_b = (jnp.where(inner, zp, zm), jnp.where(inner, 1, 7)) if bent else (zp, 1)
        rs_copy(p, slot_a, gp[p].at[cls(z2, 0)], to_a, rs_mid.at[p])
        rs_copy(p, slot_b, gp[p].at[cls(z2, 1)], to_b, rs_mid.at[p])

        def direct():
            rs_copy(p, 2, gp[p].at[cls(zp, 0)], zp, rs_root.at[pieces[p].k])
            rs_copy(p, 3, gp[p].at[cls(zm, 1)], zm, rs_root.at[pieces[p].k])

        if not bent:
            direct()
            return

        @pl.when(z < 2)
        def _():
            direct()
            rs_copy(p, 4, gp[p].at[cls(zm, 0)], zm, rs_root.at[pieces[p].k])
            rs_copy(p, 5, gp[p].at[cls(zp, 1)], zp, rs_root.at[pieces[p].k])

    def rs_forward(p):
        def forward(mid, chunk, slot, to):
            rb[p][mid] += gp[p][chunk]
            rs_copy(p, slot, rb[p].at[mid], to, rs_root.at[pieces[p].k])

        def both(count_mid):
            wait_bytes(rb[p].at[pl.ds(0, count_mid)], rs_mid.at[p])
            forward(0, cls(zm, 0), 4, zm)
            forward(1, cls(zp, 1), 5, zp)

        if not pieces[p].bent:
            both(2)
            return

        @pl.when(z >= 2)
        def _():
            both(4)
            forward(6, cls(zp, 0), 2, zp)
            forward(7, cls(zm, 1), 3, zm)

    def rs_finish(p):
        piece = pieces[p]
        mat = piece.mat
        if piece.lo == 0:
            wait_count(size_of(gf[piece.k]) // 2, rs_root.at[piece.k])
        cols = jnp.zeros((1, piece.width), jnp.float32)
        row_iota = lax.broadcasted_iota(jnp.int32, (mat.mc, LANES), 0)
        lane_iota = lax.broadcasted_iota(jnp.int32, (mat.mc, LANES), 1)
        lines = [jnp.zeros((1, LANES), jnp.float32) for _ in range(mat.rows)]
        for mirror in range(2):
            own = cls(z, mirror)
            full = gp[p][own] + rb[p][2 + mirror] + rb[p][4 + mirror]
            gf[piece.k][own, :, piece.lo:piece.lo + piece.width] = full
            sq = full * full + EPS_ONE
            cols = cols + jnp.sum(sq, axis=0, keepdims=True)
            row_part = jnp.broadcast_to(jnp.sum(sq, axis=1, keepdims=True), (mat.mc, LANES))
            first = own * mat.mc
            for a in range(mat.rows):
                hit = (row_iota + first) == (lane_iota + a * LANES)
                lines[a] = lines[a] + jnp.sum(jnp.where(hit, row_part, 0.0), axis=0, keepdims=True)
        for j in range(piece.tiles):
            at = piece.col_off + j * LANES
            c_own[at // c_len, :, at % c_len:at % c_len + LANES] = cols[:, lanes(j)]
        for a in range(mat.rows):
            at = lanes(mat.row_off + a)
            if piece.lo == 0:
                r_in[y, :, at] = lines[a]
            else:
                r_in[y, :, at] += lines[a]

    def bc_copy(k, chunk, axis_index, recv_sem):
        remote(gf[k].at[chunk], gf[k].at[chunk], bc_send, recv_sem, "dp", axis_index).start()

    last = N_MAT - 1

    def bc_part(k, chunk, rows, axis_index, send_sem, recv_sem):
        part = gf[k].at[chunk, pl.ds(*rows)]
        remote(part, part, send_sem, recv_sem, "dp", axis_index).start()

    def bc_lead(k):
        bc_copy(k, cls(z, 0), zp, bc_fwd.at[k])
        bc_copy(k, cls(z, 1), zm, bc_fwd.at[k])

    def bc_rest(k):
        near = (bc_fwd.at[0], bc_near, bc_near, bc_last)[k]
        bc_copy(k, cls(z, 1), zp, near)
        bc_copy(k, cls(z, 0), zm, near)

    half = mats[0].mc // 2

    def bc_forward(k, rows=None):
        if rows is None or rows[0] == 0:
            wait_bytes(gf[k].at[pl.ds(0, 4 if k == 0 else 2)], bc_fwd.at[k])
        far = bc_far if k == last else bc_near
        onward = ((cls(zm, 0), zp), (cls(zp, 1), zm))
        if k > 0:
            for chunk, to in onward:
                bc_part(k, chunk, rows or (0, mats[k].mc), to, bc_send, far)
            return
        for chunk, to in onward:
            bc_part(k, chunk, (0, half), to, bc_send, far)

        @pl.when(z != 3)
        def _():
            for chunk, to in onward:
                bc_part(k, chunk, (half, half), to, bc_more, far)

        @pl.when(z == 1)
        def _():
            for chunk, to in ((cls(zm, 1), zp), (cls(zp, 0), zm)):
                bc_part(k, chunk, (half, half), to, bc_more, far)

    slots = {}

    def exchange_start(e, axis, me, size, buf, scatter=None):
        slots[e] = buf.at[pl.ds(0, size - 1)]
        for d in range(1, size):
            peer = lax.rem(me + d, size)
            src = buf.at[me] if scatter is None else scatter.at[peer]
            remote(src, buf.at[me], ex_send, ex_recv.at[max(e - 1, 0)], axis, peer).start()

    def exchange_wait(e):
        if e == 0:
            wait_count(size_of(slots[0]) + size_of(slots[1]), ex_recv.at[0])
        else:
            wait_bytes(slots[e], ex_recv.at[e - 1])

    def sum_slots(buf, size):
        value = buf[0]
        for i in range(1, size):
            value = value + buf[i]
        return value

    def matmul(p):
        for t in range(pieces[p].chunks):
            matmul_chunk(p, t)

    matmul(0)
    pl.semaphore_wait(barrier, partners)
    rs_first(0)
    matmul(1)
    rs_first(1)
    matmul(2)
    rs_first(2)
    rs_forward(0)
    matmul(3)
    rs_first(3)
    matmul(4)
    rs_first(4)
    rs_forward(1)
    rs_forward(2)
    matmul(5)
    rs_first(5)
    c_own[...] = jnp.zeros_like(c_own)
    rs_finish(0)
    wait_count(sum(size_of(w) for w in w_v), w_sem)
    hyper_copy.wait()
    wait_bytes(stat_old, st_sem)
    lane = lax.broadcasted_iota(jnp.int32, (1, LANES), 1)
    scal = jnp.zeros((1, LANES), jnp.float32)
    for k in range(N_MAT):
        for mirror in range(2):
            own_w = w_v[k][cls(z, mirror)]
            scal = jnp.where(lane == 4 + k, scal + total(own_w * own_w), scal)
    rs_forward(3)
    rs_finish(1)
    rs_finish(2)
    rs_forward(4)
    rs_forward(5)
    bc_lead(0)
    bc_rest(0)
    rs_finish(3)
    rs_finish(4)
    bc_lead(1)
    bc_rest(1)
    rs_finish(5)
    c_in[x] = c_own[x]
    exchange_start(0, "row", x, row_size, c_in, c_own)
    exchange_start(1, "col", y, col_size, r_in)
    exchange_wait(0)
    z_in[z, :, 0:c_len] = sum_slots(c_in, row_size)
    r_own[...] = sum_slots(r_in, col_size)
    for i, line in enumerate(own_lines(z)):
        z_in[z, :, c_len + i * LANES:c_len + (i + 1) * LANES] = r_own[:, pl.ds(pl.multiple_of(line * LANES, LANES), LANES)]
    exchange_start(2, "dp", z, dp_size, z_in)
    bc_forward(0)
    bc_lead(2)
    bc_rest(2)
    exchange_wait(2)
    sums = z_in[0, :, 0:c_len]
    for i in range(1, dp_size):
        sums = sums + z_in[i, :, 0:c_len]
    c_all[x] = sums

    def z_line(i, slot):
        return z_in[i, :, c_len + slot * LANES:c_len + (slot + 1) * LANES]

    def row_line(k, a):
        if k < last:
            return z_line(2 * a, k) + z_line(2 * a + 1, k)
        parts = ([z_line(a, last)] if a < dp_size else []) + ([z_line(a - 1, last + 1)] if a > 0 else [])
        return parts[0] + parts[1] if len(parts) == 2 else parts[0]

    exchange_start(3, "row", x, row_size, c_all)
    bc_forward(1, (0, 3 * mats[1].mc // 4))
    beta_two, rho_step, clip_thr = hyper[0], hyper[1], hyper[2]
    row_iota = lax.broadcasted_iota(jnp.int32, (LANES, LANES), 0)
    lane_iota = lax.broadcasted_iota(jnp.int32, (LANES, LANES), 1)
    eye = row_iota == lane_iota
    local_sum = []
    for k, mat in enumerate(mats):
        lines = []
        for a in range(mat.rows):
            at = mat.row_off + a
            mean = row_line(k, a) * (1.0 / mat.n_total)
            lines.append(beta_two * stat_old[:, lanes(at)] + (1.0 - beta_two) * mean)
            stat_new[:, lanes(at)] = lines[-1]
        s_loc = lines[0]
        for line in lines[1:]:
            s_loc = s_loc + line
        s_loc = jnp.sum(s_loc, axis=1, keepdims=True)
        local_sum.append(s_loc)
        for a in range(mat.rows):
            scaled = lax.rsqrt(lines[a] / s_loc)
            column = jnp.sum(jnp.where(eye, jnp.broadcast_to(scaled, (LANES, LANES)), 0.0), axis=1, keepdims=True)
            acol[k][pl.ds(a * LANES, LANES), :] = jnp.broadcast_to(column, (LANES, LANES))
    exchange_wait(3)
    for k, mat in enumerate(mats):
        for j in range(mat.n // LANES):
            at = mat.col_off + j * LANES
            mean = c_all[at // c_len, :, at % c_len:at % c_len + LANES] * (1.0 / mat.m_total)
            new_c = beta_two * stat_old[:, n_row + at:n_row + at + LANES] + (1.0 - beta_two) * mean
            stat_new[:, n_row + at:n_row + at + LANES] = new_c
            b_row[:, at:at + LANES] = lax.rsqrt(new_c)

    def scaled_tile(k, chunk, j):
        mat = mats[k]
        rows = pl.ds(pl.multiple_of(chunk * mat.mc, 8), mat.mc)
        cols = b_row[:, mat.col_off + j * LANES:mat.col_off + (j + 1) * LANES]
        return gf[k][chunk, :, lanes(j)] * acol[k][rows, :] * cols

    for k, mat in enumerate(mats):
        acc = jnp.zeros((mat.mc, LANES), jnp.float32)
        for mirror in range(2):
            for j in range(mat.n // LANES):
                upd = scaled_tile(k, cls(z, mirror), j)
                acc = acc + upd * upd
        scal = jnp.where(lane == k, total(acc), scal)
    sz[z] = scal
    exchange_start(4, "dp", z, dp_size, sz)
    bc_forward(1, (3 * mats[1].mc // 4, mats[1].mc // 4))
    bc_lead(3)
    bc_rest(3)
    bc_forward(2)
    exchange_wait(4)
    sy[y] = sum_slots(sz, dp_size)
    exchange_start(5, "col", y, col_size, sy)
    bc_forward(3)
    exchange_wait(5)
    scal = sum_slots(sy, col_size)
    for k in range(N_MAT):
        scal = jnp.where(lane == 8 + k, jnp.broadcast_to(local_sum[k], (1, LANES)), scal)
    sx[x] = scal
    exchange_start(6, "row", x, row_size, sx)
    exchange_wait(6)
    table = jnp.concatenate([sx[i] for i in range(row_size)], axis=0)
    t_lane = lax.broadcasted_iota(jnp.int32, (row_size, LANES), 1)

    def pick(at):
        return jnp.sum(jnp.where(t_lane == at, table, 0.0), axis=1, keepdims=True)

    factors = []
    for k, mat in enumerate(mats):
        s_each = pick(8 + k)
        s_all = jnp.sum(s_each, axis=0, keepdims=True)
        count = 1.0 / (mat.m_total * mat.n_total)
        u_sq = jnp.sum((s_all / s_each) * pick(k), axis=0, keepdims=True)
        w_sq = jnp.sum(pick(4 + k), axis=0, keepdims=True)
        u_rms = jnp.sqrt(u_sq * count)
        w_rms = jnp.sqrt(w_sq * count)
        step = rho_step * jnp.maximum(EPS_TWO, w_rms) / jnp.maximum(1.0, u_rms / clip_thr)
        factors.append(step * jnp.sqrt(s_all / local_sum[k]))

    moved = sum(size_of(g) for g in gf) * 6 // 8

    def update(k, chunk):
        for j in range(mats[k].n // LANES):
            w_v[k][chunk, :, lanes(j)] = w_v[k][chunk, :, lanes(j)] - factors[k] * scaled_tile(k, chunk, j)

    for k in range(N_MAT):
        for chunk in (cls(z, 0), cls(z, 1), cls(zm, 0), cls(zp, 1)):
            update(k, chunk)
    wait_count(sum(size_of(gf[k].at[pl.ds(0, 2 if k == 0 else 4)]) for k in range(last)), bc_near)
    wait_bytes(gf[last].at[pl.ds(0, 2)], bc_last)
    for k in range(N_MAT):
        update(k, cls(zm, 1))
        update(k, cls(zp, 0))
        if k == last:
            wait_count(moved, rs_send)
            wait_count(sum(size_of(slot) for slot in slots.values()), ex_send)
            wait_bytes(gf[k].at[pl.ds(0, 2)], bc_far)
        update(k, cls(z2, 0))
        update(k, cls(z2, 1))
    chunk_size = size_of(gf[0].at[0])
    wait_count(moved - chunk_size, bc_send)

    @pl.when(z == 1)
    def _():
        wait_count(2 * chunk_size, bc_more)

    @pl.when((z == 0) | (z == 2))
    def _():
        wait_count(chunk_size, bc_more)


def write_kernel(mats, w0, w1, w2, w3, stat_new,
                 o0, o1, o2, o3, ro0, ro1, ro2, ro3, co0, co1, co2, co3, w_sem, r_sem, c_sem):
    n_row = sum(mat.m for mat in mats)
    copies = [pltpu.make_async_copy(src, dst, w_sem.at[k])
              for k, (src, dst) in enumerate(zip((w0, w1, w2, w3), (o0, o1, o2, o3)))]
    for k, mat in enumerate(mats):
        r_out = (ro0, ro1, ro2, ro3)[k]
        c_out = (co0, co1, co2, co3)[k]
        copies.append(pltpu.make_async_copy(stat_new.at[0, pl.ds(mat.row_off * LANES, mat.m)], r_out, r_sem.at[k]))
        copies.append(pltpu.make_async_copy(stat_new.at[0, pl.ds(n_row + mat.col_off, mat.n)], c_out, c_sem.at[k]))
    for copy in copies:
        copy.start()
    for copy in copies:
        copy.wait()


def fused_step(mats, dp_size, col_size, row_size, args):
    (x_attn, dy_attn, x_mlp, dy_gate, dy_up, h_mlp, dy_out, w_list, r_list, c_list, hyper) = args
    any_spec = pl.BlockSpec(memory_space=pl.ANY)
    vmem_spec = pl.BlockSpec(memory_space=pltpu.VMEM)
    f32 = jnp.float32
    pieces = []
    for k, tiles, chunks, bent in PIECES:
        lo = sum(piece.width for piece in pieces if piece.k == k)
        pieces.append(Piece(k, mats[k], lo, tiles * LANES, chunks, bent))
    n_p = len(pieces)
    w_in = [w.reshape(8, mat.mc, mat.n) for w, mat in zip(w_list, mats)]
    acts = (x_attn, dy_attn, x_mlp, dy_gate, dy_up, h_mlp, dy_out)
    n_row = sum(mat.m for mat in mats)
    n_col = sum(mat.n for mat in mats)
    c_len = -(-n_col // (row_size * LANES)) * LANES
    w_shape = [jax.ShapeDtypeStruct(w.shape, f32) for w in w_in]
    held_shape = [pltpu.VMEM(w.shape, f32) for w in w_in] + [pltpu.VMEM((1, n_row + n_col), f32)]
    dma = pltpu.SemaphoreType.DMA
    n_load = sum(piece.chunks for piece in pieces)
    scratch = ([pltpu.VMEM(a.shape, a.dtype) for a in acts]
               + [pltpu.VMEM(x_attn.shape[::-1], x_attn.dtype)]
               + [pltpu.VMEM((8, piece.mc, piece.width), f32) for piece in pieces]
               + [pltpu.VMEM((8 if piece.bent else 6, piece.mc, piece.width), f32) for piece in pieces]
               + [pltpu.VMEM((8, mat.mc, mat.n), f32) for mat in mats]
               + [pltpu.VMEM((mat.m, LANES), f32) for mat in mats]
               + [pltpu.SMEM((3,), f32), pltpu.VMEM((1, n_row + n_col), f32), pltpu.VMEM((1, n_col), f32),
                  pltpu.VMEM((row_size, 1, c_len), f32), pltpu.VMEM((row_size, 1, c_len), f32),
                  pltpu.VMEM((col_size, 1, n_row), f32), pltpu.VMEM((1, n_row), f32),
                  pltpu.VMEM((dp_size, 1, c_len + (N_MAT + 1) * LANES), f32),
                  pltpu.VMEM((row_size, 1, c_len), f32),
                  pltpu.VMEM((dp_size, 1, LANES), f32), pltpu.VMEM((col_size, 1, LANES), f32),
                  pltpu.VMEM((row_size, 1, LANES), f32)]
               + [pltpu.VMEM((256, 1, LANES), f32)]
               + [dma((n_load,)), dma(()), dma(()), dma(()),
                  dma(()), dma((n_p,)), dma((N_MAT,)),
                  dma(()), dma((N_MAT,)), dma(()), dma(()), dma(()), dma(()),
                  dma(()), dma((6,))])
    held = pl.pallas_call(
        functools.partial(kernel, mats, pieces, dp_size, col_size, row_size),
        out_shape=held_shape,
        in_specs=[any_spec] * 20,
        out_specs=[vmem_spec] * 5,
        scratch_shapes=scratch,
        compiler_params=pltpu.CompilerParams(collective_id=0, has_side_effects=True, vmem_limit_bytes=VMEM_LIMIT),
        name="adafactor_step",
    )(*acts, *w_in, *r_list, *c_list, hyper)
    outs = pl.pallas_call(
        functools.partial(write_kernel, mats),
        out_shape=(w_shape + [jax.ShapeDtypeStruct(r.shape, f32) for r in r_list]
                   + [jax.ShapeDtypeStruct(c.shape, f32) for c in c_list]),
        in_specs=[vmem_spec] * 5,
        out_specs=[any_spec] * 12,
        scratch_shapes=[dma((N_MAT,)), dma((N_MAT,)), dma((N_MAT,))],
        compiler_params=pltpu.CompilerParams(vmem_limit_bytes=WRITE_LIMIT),
        name="write_out",
    )(*held)
    new_w = [o.reshape(w.shape) for o, w in zip(outs[:4], w_list)]
    return tuple(part for trio in zip(new_w, outs[4:8], outs[8:]) for part in trio)


def solution(mesh):
    row_size = mesh.shape['row']
    col_size = mesh.shape['col']
    dp_size = mesh.shape['dp']
    act_spec = P('dp', 'row')
    grad_spec = P('dp', 'col')
    w_spec = P('row', 'col')
    row_spec = P('row')
    col_spec = P('col')
    in_specs = (act_spec, grad_spec, act_spec, grad_spec, grad_spec, act_spec, grad_spec,
                w_spec, w_spec, w_spec, w_spec,
                row_spec, col_spec, row_spec, col_spec, row_spec, col_spec, row_spec, col_spec, P())
    out_specs = (w_spec, row_spec, col_spec) * 4

    def per_device(x_attn, dy_attn, x_mlp, dy_gate, dy_up, h_mlp, dy_out, w_attn, w_gate, w_up, w_down,
                   r_attn, c_attn, r_gate, c_gate, r_up, c_up, r_down, c_down, hyper_params):
        w_list = (w_attn, w_gate, w_up, w_down)
        mats = []
        row_off = col_off = 0
        for w in w_list:
            mats.append(Mat(w.shape[0], w.shape[1], row_size, col_size, row_off, col_off))
            row_off += mats[-1].rows
            col_off += mats[-1].n
        return fused_step(mats, dp_size, col_size, row_size,
                          (x_attn, dy_attn, x_mlp, dy_gate, dy_up, h_mlp, dy_out, w_list,
                           (r_attn, r_gate, r_up, r_down), (c_attn, c_gate, c_up, c_down), hyper_params))

    return jax.shard_map(per_device, mesh=mesh, in_specs=in_specs, out_specs=out_specs, check_vma=False)
```
